32 devices in a mesh: panel: 4 (over y, x), tile: 8 (over z, core).
Axes of the slice: x: 2, y: 2, z: 4, core: 2. Of those that a mesh axis runs over, the one named last changes fastest.
Arguments:
- snapshots: bfloat16 [32, 64, 2, 512], P('panel', 'tile'), may hold values from -24 to 24
- beam_codes: int32 [32, 64], P(None, 'tile'), may hold values from 0 to 63
- panel_codes: int32 [32], replicated, may hold values from 0 to 63
- loading: float32 [32], P('panel'), may hold values from 1 to 10
Outputs:
- cancel: float32 [32, 62, 2], P('panel')
- beam_out: float32 [2, 512], P(None, 'tile')
The draws below stay inside these ranges and needn't reach their ends.
All inputs are finite; a program needn't handle non-finite values.
Results may differ from the reference program's by a relative error of at most 0.0036.
Values may be sent and summed in bfloat16 or wider, within the bound.
A program may use at most 64 MiB of HBM per device.

```python
import math
import jax
import jax.numpy as jnp
from jax import lax

BEAMS = 32
SNAPS = 512
INTERFERERS = 40
PANELS = 32
TILES = 64


def draw_snapshots(key, part):
    key_dir, key_amp, key_sig, key_noise = jax.random.split(jax.random.fold_in(key, 17), 4)
    elements = PANELS * TILES
    direction = jax.random.uniform(key_dir, (INTERFERERS,), minval=-1.0, maxval=1.0)
    amplitude = jax.random.uniform(key_amp, (INTERFERERS,), minval=0.2, maxval=0.6)
    position = jnp.arange(elements, dtype=jnp.float32)
    phase = jnp.pi * direction[:, None] * position[None, :]
    along_real = jnp.cos(phase)
    along_imag = jnp.sin(phase)
    signal = jax.random.normal(key_sig, (2, INTERFERERS, SNAPS), jnp.float32) * amplitude[None, :, None]
    real_part = jnp.dot(along_real.T, signal[0], precision=lax.Precision.HIGHEST) - jnp.dot(along_imag.T, signal[1], precision=lax.Precision.HIGHEST)
    imag_part = jnp.dot(along_imag.T, signal[0], precision=lax.Precision.HIGHEST) + jnp.dot(along_real.T, signal[1], precision=lax.Precision.HIGHEST)
    noise = jax.random.normal(key_noise, (elements, 2, SNAPS), jnp.float32)
    values = jnp.stack([real_part, imag_part], axis=1) + noise
    values = jnp.clip(values, -24.0, 24.0)
    return values.reshape(PANELS, TILES, 2, SNAPS).astype(jnp.bfloat16)


def plant(drawn, key, least, top_value):
    longest = drawn.shape.index(max(drawn.shape))
    spots = []
    for shift in (0, 1):
        where = [jax.random.randint(jax.random.fold_in(key, axis), (), 0, length) for axis, length in enumerate(drawn.shape)]
        where[longest] = (where[longest] + shift) % drawn.shape[longest]
        spots.append(tuple(where))
    return drawn.at[spots[0]].set(least).at[spots[1]].set(top_value)


def shard_levels(own_key, dims, cuts, least, largest):
    gain = 1.0
    for dim, blocks in cuts:
        heights = jax.random.uniform(jax.random.fold_in(jax.random.fold_in(own_key, 6), dim), (blocks,), jnp.float32, least / len(cuts), largest / len(cuts))
        gain = gain * jnp.repeat(jnp.exp(heights), dims[dim] // blocks).reshape((-1,) + (1,) * (len(dims) - 1 - dim))
    return gain


def setup_inputs(seed: int = 0) -> dict:
    splits = jax.random.split(jax.random.key(seed), 5)
    return {
        "snapshots": draw_snapshots(jax.random.fold_in(splits[4], 71), 0),
        "beam_codes": plant(jax.random.randint(splits[1], (BEAMS, TILES), 0, 64), jax.random.fold_in(splits[1], 1), 0, 63).astype(jnp.int32),
        "panel_codes": plant(jax.random.randint(splits[2], (PANELS,), 0, 64), jax.random.fold_in(splits[2], 1), 0, 63).astype(jnp.int32),
        "loading": jnp.clip(jnp.exp(math.log(10.0) - 2.3025851 * jax.random.uniform(splits[3], (PANELS,), jnp.float32) ** shard_levels(splits[3], (PANELS,), ((0, 4),), -0.2, 0.2)), 1.0, 10.0),
    }


phase_levels = 64
array_load = 1.0

def steering_rows(codes, total_tiles):
    angles = codes.astype(jnp.float32) * (2.0 * math.pi / phase_levels)
    cosine = jnp.cos(angles)
    sine = jnp.sin(angles)
    count_beams = codes.shape[0]
    count_tiles = codes.shape[1]
    real_rows = jnp.stack([cosine, sine], axis=-1).reshape(count_beams, 2 * count_tiles)
    imag_rows = jnp.stack([-sine, cosine], axis=-1).reshape(count_beams, 2 * count_tiles)
    table = jnp.stack([real_rows, imag_rows], axis=1).reshape(2 * count_beams, 2 * count_tiles)
    return (table / math.sqrt(total_tiles)).astype(jnp.bfloat16)

def solve_one(factor_one, right_one):
    return jax.scipy.linalg.cho_solve((factor_one, True), right_one)

def cancel_weights(covar):
    factor = jnp.linalg.cholesky(covar[:, 2:, 2:])
    return jax.vmap(solve_one)(factor, covar[:, 2:, :2])

def constraint_matrix(panel_codes):
    angles = panel_codes.astype(jnp.float32) * (2.0 * math.pi / phase_levels)
    cosine = jnp.cos(angles)
    sine = jnp.sin(angles)
    upper = jnp.stack([cosine, -sine], axis=-1)
    lower = jnp.stack([sine, cosine], axis=-1)
    return jnp.stack([upper, lower], axis=1).reshape(2 * panel_codes.shape[0], 2)

def array_weights(covar, constraint):
    factor = jnp.linalg.cholesky(covar)
    solved = jax.scipy.linalg.cho_solve((factor, True), constraint)
    gram = jnp.dot(constraint.T, solved, precision=lax.Precision.HIGHEST)
    determinant = gram[0, 0] * gram[1, 1] - gram[0, 1] * gram[1, 0]
    inverse = jnp.stack([jnp.stack([gram[1, 1], -gram[0, 1]]), jnp.stack([-gram[1, 0], gram[0, 0]])]) / determinant
    return jnp.dot(solved, inverse, precision=lax.Precision.HIGHEST)

def reference(snapshots, beam_codes, panel_codes, loading):
    table = steering_rows(beam_codes, TILES)
    samples = snapshots.reshape(PANELS, 2 * TILES, SNAPS).astype(jnp.float32)
    beams = jnp.einsum('bk,pks->pbs', table.astype(jnp.float32), samples, precision=lax.Precision.HIGHEST)
    width = 2 * BEAMS
    covar = jnp.einsum('pis,pjs->pij', beams, beams, precision=lax.Precision.HIGHEST) / SNAPS
    covar = covar + loading[:, None, None] * jnp.eye(width, dtype=jnp.float32)[None, :, :]
    cancel = cancel_weights(covar)
    outputs = beams[:, :2, :] - jnp.einsum('pak,pas->pks', cancel, beams[:, 2:, :], precision=lax.Precision.HIGHEST)
    flat = outputs.reshape(2 * PANELS, SNAPS)
    array_covar = jnp.dot(flat, flat.T, precision=lax.Precision.HIGHEST) / SNAPS
    array_covar = array_covar + array_load * jnp.eye(2 * PANELS, dtype=jnp.float32)
    weights = array_weights(array_covar, constraint_matrix(panel_codes))
    beam_out = jnp.dot(weights.T, flat, precision=lax.Precision.HIGHEST) * math.sqrt(PANELS)
    return (cancel, beam_out)
```

```python
import functools
import math

import jax
import jax.numpy as jnp
from jax import lax
from jax.experimental import pallas as pl
from jax.experimental.pallas import tpu as pltpu
from jax.sharding import PartitionSpec as P

MESH = pl.DeviceIdType.MESH
LANES = 128
SUBS = 8
UNROLL1 = 2
UNROLL2 = 2
HIGH = lax.Precision.HIGHEST

phase_levels = 64
array_load = 1.0


def steering_rows(codes, total_tiles):
    angles = codes.astype(jnp.float32) * (2.0 * math.pi / phase_levels)
    cosine = jnp.cos(angles)
    sine = jnp.sin(angles)
    count_beams = codes.shape[0]
    count_tiles = codes.shape[1]
    real_rows = jnp.stack([cosine, sine], axis=-1).reshape(count_beams, 2 * count_tiles)
    imag_rows = jnp.stack([-sine, cosine], axis=-1).reshape(count_beams, 2 * count_tiles)
    table = jnp.stack([real_rows, imag_rows], axis=1).reshape(2 * count_beams, 2 * count_tiles)
    return (table / math.sqrt(total_tiles)).astype(jnp.bfloat16)


def solve_one(factor_one, right_one):
    return jax.scipy.linalg.cho_solve((factor_one, True), right_one)


def cancel_weights(covar):
    factor = jnp.linalg.cholesky(covar[:, 2:, 2:])
    return jax.vmap(solve_one)(factor, covar[:, 2:, :2])


def constraint_matrix(panel_codes):
    angles = panel_codes.astype(jnp.float32) * (2.0 * math.pi / phase_levels)
    cosine = jnp.cos(angles)
    sine = jnp.sin(angles)
    upper = jnp.stack([cosine, -sine], axis=-1)
    lower = jnp.stack([sine, cosine], axis=-1)
    return jnp.stack([upper, lower], axis=1).reshape(2 * panel_codes.shape[0], 2)


def array_weights(covar, constraint):
    factor = jnp.linalg.cholesky(covar)
    solved = jax.scipy.linalg.cho_solve((factor, True), constraint)
    gram = jnp.dot(constraint.T, solved, precision=HIGH)
    determinant = gram[0, 0] * gram[1, 1] - gram[0, 1] * gram[1, 0]
    inverse = (
        jnp.stack([jnp.stack([gram[1, 1], -gram[0, 1]]), jnp.stack([-gram[1, 0], gram[0, 0]])])
        / determinant
    )
    return jnp.dot(solved, inverse, precision=HIGH)


def plain_body(snapshots, beam_codes, panel_codes, loading):
    own_panels, own_tiles, _, snaps = snapshots.shape
    tile_count = lax.axis_size("tile")
    block_snaps = snaps // tile_count
    table = steering_rows(beam_codes, own_tiles * tile_count)
    samples = snapshots.reshape(own_panels, 2 * own_tiles, snaps)
    partial_value = jnp.einsum("bk,pks->pbs", table, samples, preferred_element_type=jnp.float32)
    totals = lax.psum(partial_value, "tile")
    summed = jnp.einsum("pis,pjs->pij", totals, totals, precision=HIGH)
    start = lax.axis_index("tile") * block_snaps
    beams = lax.dynamic_slice_in_dim(totals, start, block_snaps, 2)
    identity = jnp.eye(beams.shape[1], dtype=jnp.float32)
    covar = summed / snaps + loading[:, None, None] * identity[None, :, :]
    cancel = cancel_weights(covar)
    outputs = beams[:, :2, :] - jnp.einsum("pak,pas->pks", cancel, beams[:, 2:, :], precision=HIGH)
    gathered = lax.all_gather(outputs, "panel", axis=0, tiled=True)
    flat = gathered.reshape(gathered.shape[0] * 2, block_snaps)
    array_sum = lax.psum(jnp.dot(flat, flat.T, precision=HIGH), "tile")
    array_covar = array_sum / snaps + array_load * jnp.eye(flat.shape[0], dtype=jnp.float32)
    weights = array_weights(array_covar, constraint_matrix(panel_codes))
    beam_out = jnp.dot(weights.T, flat, precision=HIGH) * math.sqrt(flat.shape[0] // 2)
    return (cancel, beam_out)


def iota(shape, dim):
    return lax.broadcasted_iota(jnp.int32, shape, dim)


def cos_code(code):
    code = code & (phase_levels - 1)
    eighth = phase_levels // 8
    quarter = phase_levels // 4
    quadrant = ((code + eighth) >> 4) & 3
    rest = code - (((code + eighth) >> 4) * quarter)
    x = rest.astype(jnp.float32) * (2.0 * math.pi / phase_levels)
    y = x * x
    cosine = 1.0 + y * (-0.5 + y * (1 / 24 + y * (-1 / 720 + y * (1 / 40320 - y * (1 / 3628800)))))
    sine = x * (1.0 + y * (-1 / 6 + y * (1 / 120 + y * (-1 / 5040 + y * (1 / 362880)))))
    odd = (quadrant & 1) == 1
    flip = jnp.where((quadrant == 1) | (quadrant == 2), -1.0, 1.0)
    return jnp.where(odd, sine, cosine) * flip


def contract(a, b, dims, precision=HIGH):
    return lax.dot_general(a, b, (dims, ((), ())), precision=precision, preferred_element_type=jnp.float32)


def far_first(own, count):
    order = []
    for k in range(count - 1):
        down = count - 1 - k
        down = jnp.where(down <= own, down - 1, down)
        up = jnp.where(k >= own, k + 1, k)
        order.append(jnp.where(own < count // 2, down, up))
    return order


def eliminate(rows, unroll):
    width = rows[0].shape[1]
    sub = iota((SUBS, width), 0)
    spread = lambda row: jnp.broadcast_to(row, (SUBS, width))

    def block(base, rows):
        def column(value, j):
            return jnp.take_along_axis(value, jnp.full((SUBS, width), base + j, jnp.int32), axis=1)

        group, others = rows[0], list(rows[1:])
        diag = [column(group, j) for j in range(SUBS)]
        factors = [[column(value, j) for value in others] for j in range(SUBS)]
        for j in range(SUBS):
            scale = 1.0 / spread(diag[j][j : j + 1])
            here = sub == j
            lead = diag[j] * scale

            def reduce(value):
                row = spread(value[j : j + 1])
                return jnp.where(here, row * scale, value - lead * row)

            for k in range(j + 1, SUBS):
                diag[k] = reduce(diag[k])
            group = reduce(group)
        spreads = [spread(group[j : j + 1]) for j in range(SUBS)]
        for r in range(len(others)):
            terms = [factors[j][r] * spreads[j] for j in range(SUBS)]
            while len(terms) > 1:
                terms = [sum(terms[i : i + 2][1:], terms[i]) for i in range(0, len(terms), 2)]
            others[r] = others[r] - terms[0]
        return others + [group]

    def step(index, rows):
        for u in range(unroll):
            rows = block((index * unroll + u) * SUBS, rows)
        return tuple(rows)

    steps = len(rows) // unroll
    if steps == 1:
        return list(step(0, rows))
    return list(lax.fori_loop(0, steps, step, tuple(rows)))


def fused_kernel(
    sizes, loading_in, snaps_in, codes_in, panel_codes_in, cancel_out, beam_out,
    loading, panel_codes, own, got, codes_own, codes_got, flat, cancels,
    local_sem, send_a, recv_a, send_c, recv_c, send_f, recv_f, send_w, recv_w,
):
    panel_count, tile_count, total_panels = sizes
    own_panels, own_tiles, _, snaps = snaps_in.shape
    total_tiles = own_tiles * tile_count
    beams_count = codes_in.shape[1]
    width = 2 * beams_count
    chunks = snaps // LANES
    pi, ti = lax.axis_index("panel"), lax.axis_index("tile")
    devices = panel_count * tile_count

    peers = []
    for dp in range(panel_count):
        for dt in range(tile_count):
            if dp or dt:
                peers.append((dp, dt))
    there = lambda dp, dt: (lax.rem(pi + dp, panel_count), lax.rem(ti + dt, tile_count))
    back = lambda dp, dt: (
        lax.rem(pi + panel_count - dp, panel_count),
        lax.rem(ti + tile_count - dt, tile_count),
    )

    barrier = pltpu.get_barrier_semaphore()
    near = [(dp, dt) for dp, dt in peers if not (dp and dt)]
    for dp, dt in near:
        pl.semaphore_signal(barrier, inc=1, device_id=there(dp, dt), device_id_type=MESH)
    loads = [
        pltpu.make_async_copy(source, target, local_sem.at[index])
        for index, (source, target) in enumerate((
            (codes_in, codes_own),
            (snaps_in, own),
            (snaps_in.at[ti], got.at[ti]),
            (codes_in, codes_got.at[ti]),
            (loading_in, loading),
            (panel_codes_in, panel_codes),
        ))
    ]
    for load in loads:
        load.start()
    for load in loads:
        load.wait()
    pl.semaphore_wait(barrier, len(near))

    tiles = far_first(ti, tile_count)
    panels = far_first(pi, panel_count)
    waits = []
    for k, other in enumerate(tiles, 1):
        piece = pltpu.make_async_remote_copy(
            codes_own, codes_got.at[ti], send_c.at[k], recv_c.at[ti], device_id=(pi, other), device_id_type=MESH
        )
        piece.start()
        arrival = pltpu.make_async_remote_copy(
            codes_own, codes_got.at[other], send_c.at[k], recv_c.at[other], device_id=(pi, other), device_id_type=MESH
        )
        waits.append((piece, arrival))
    bulk = []
    for k, other in enumerate(tiles, 1):
        piece = pltpu.make_async_remote_copy(
            own.at[other], got.at[ti], send_a.at[k], recv_a.at[ti], device_id=(pi, other), device_id_type=MESH
        )
        piece.start()
        arrival = pltpu.make_async_remote_copy(
            own.at[other], got.at[other], send_a.at[k], recv_a.at[other], device_id=(pi, other), device_id_type=MESH
        )
        bulk.append((piece, arrival))

    order = 2 * total_panels
    code_row = jnp.broadcast_to(panel_codes[...], (order, total_panels))
    own_code = jnp.where(iota((order, total_panels), 1) == lax.rem(iota((order, total_panels), 0), total_panels), code_row, 0)
    code_col = jnp.broadcast_to(jnp.sum(own_code, axis=1, keepdims=True), (order, LANES))
    lower = iota((order, LANES), 0) >= total_panels
    lane = iota((order, LANES), 1)
    quarter = phase_levels // 4
    shift = jnp.where(lane == 0, jnp.where(lower, -quarter, 0), jnp.where(lower, 0, quarter))
    constraint = jnp.where(lane < 2, cos_code(code_col + shift), 0.0)

    for piece, arrival in waits:
        arrival.wait_recv()
    codes_all = codes_got[...].reshape(total_tiles, beams_count).astype(jnp.float32)
    k_rows = (iota((2 * total_tiles, total_tiles), 0) >> 1) == iota((2 * total_tiles, total_tiles), 1)
    beam_of = lambda index: lax.rem(index + 2, width)
    b_cols = (beam_of(iota((beams_count, width), 1)) >> 1) == iota((beams_count, width), 0)
    tall = contract(k_rows.astype(jnp.bfloat16), codes_all.astype(jnp.bfloat16), ((1,), (0,)), None)
    wide = contract(tall.astype(jnp.bfloat16), b_cols.astype(jnp.bfloat16), ((1,), (0,)), None)
    code = (wide + 0.5).astype(jnp.int32)
    k_odd = iota(code.shape, 0) & 1
    i_odd = iota(code.shape, 1) & 1
    table = cos_code(code + quarter * (i_odd - k_odd)) / math.sqrt(total_tiles)
    table = table.astype(jnp.bfloat16)

    for piece, arrival in bulk:
        arrival.wait_recv()
    samples = got[...].reshape(2 * total_tiles, snaps)
    beams = contract(table, samples, ((0,), (0,)), None)
    covar = contract(beams, beams, ((1,), (1,))) / snaps
    diagonal = iota((width, width), 0) == iota((width, width), 1)
    covar = covar + jnp.where(diagonal, loading[ti], 0.0)
    row, col = iota((width, width), 0), iota((width, width), 1)
    inside = (row < width - 2) & (col < width - 2)
    full = jnp.concatenate([jnp.where(inside, covar, jnp.where(diagonal, 1.0, 0.0)), covar], axis=1)
    groups = eliminate([full[r : r + SUBS] for r in range(0, width, SUBS)], UNROLL1)
    solved = jnp.concatenate(groups, axis=0)[:, width:]
    mix = jnp.where(iota((width, width), 0) < width - 2, -solved, jnp.where(diagonal, 1.0, 0.0))
    outputs = contract(mix, beams, ((0,), (0,)))
    own_panel = pi * own_panels + ti
    for j in range(chunks):
        flat[own_panel, 2 * j : 2 * j + 2, :] = outputs[width - 2 :, j * LANES : (j + 1) * LANES]

    arrivals = []
    targets = [(p, t) for t in tiles for p in panels + [pi]] + [(p, ti) for p in panels]
    for k, to in enumerate(targets):
        slot = to[0] * own_panels + to[1]
        piece = pltpu.make_async_remote_copy(
            flat.at[own_panel], flat.at[own_panel], send_f.at[k], recv_f.at[own_panel],
            device_id=to, device_id_type=MESH,
        )
        piece.start()
        arrival = pltpu.make_async_remote_copy(
            flat.at[slot], flat.at[slot], send_f.at[k], recv_f.at[slot],
            device_id=to, device_id_type=MESH,
        )
        arrivals.append((piece, arrival))
    side = mix.T[width - 2 :, :]
    cancels[ti, :, :width] = -side
    passes = []
    for dt in range(1, tile_count):
        to = there(0, dt)
        source = back(0, dt)[1]
        piece = pltpu.make_async_remote_copy(
            cancels.at[ti], cancels.at[ti], send_w.at[dt], recv_w.at[ti], device_id=to, device_id_type=MESH
        )
        piece.start()
        arrival = pltpu.make_async_remote_copy(
            cancels.at[source], cancels.at[source], send_w.at[dt], recv_w.at[source], device_id=to, device_id_type=MESH
        )
        passes.append((piece, arrival))

    for piece, arrival in arrivals:
        arrival.wait_recv()
    pick = lambda row: flat[:, pl.ds(row, 1), :].reshape(total_panels, LANES)
    parts = [jnp.concatenate([flat[:, 2 * j, :], flat[:, 2 * j + 1, :]], axis=0) for j in range(chunks)]
    array_covar = contract(parts[0], parts[0], ((1,), (1,)))
    for part in parts[1:]:
        array_covar = array_covar + contract(part, part, ((1,), (1,)))
    eye = jnp.where(iota((order, order), 0) == iota((order, order), 1), array_load, 0.0)
    array_covar = array_covar / snaps + eye
    full = jnp.concatenate([array_covar, constraint[:, : LANES - order]], axis=1)
    groups = eliminate([full[r : r + SUBS] for r in range(0, order, SUBS)], UNROLL2)
    solved = jnp.concatenate(groups, axis=0)[:, order:]
    block = snaps // tile_count
    per = LANES // block
    chunk = ti // per
    mine = parts[0]
    for j in range(1, chunks):
        mine = jnp.where(chunk == j, parts[j], mine)
    joint = contract(solved, jnp.concatenate([mine, constraint], axis=1), ((0,), (0,)))[:SUBS]
    gram_t = joint[:, LANES : LANES + 2]
    g00, g01 = gram_t[0:1, 0:1], gram_t[1:2, 0:1]
    g10, g11 = gram_t[0:1, 1:2], gram_t[1:2, 1:2]
    scale = math.sqrt(total_panels) / (g00 * g11 - g01 * g10)
    s0, s1 = joint[0:1, :LANES], joint[1:2, :LANES]
    row0 = (g11 * s0 - g10 * s1) * scale
    row1 = (g00 * s1 - g01 * s0) * scale
    both = jnp.concatenate([row0, row1], axis=0)
    spot = lax.rem(ti, per)
    chosen = both[:, :block]
    for j in range(1, per):
        chosen = jnp.where(spot == j, both[:, j * block : (j + 1) * block], chosen)
    beam_out[...] = chosen

    for piece, arrival in passes:
        arrival.wait_recv()
    for piece, arrival in waits + bulk + arrivals + passes:
        piece.wait_send()
    cancel_out[...] = cancels[:, :, : width - 2]


def fused_body(panel_count, tile_count, snapshots, beam_codes, panel_codes, loading):
    own_panels, own_tiles, _, snaps = snapshots.shape
    beams_count = beam_codes.shape[0]
    total_panels = own_panels * panel_count
    dma = pltpu.SemaphoreType.DMA
    devices = panel_count * tile_count
    any_space = pl.BlockSpec(memory_space=pl.ANY)
    vmem = pl.BlockSpec(memory_space=pltpu.VMEM)
    cancel_t, beam_out = pl.pallas_call(
        functools.partial(fused_kernel, (panel_count, tile_count, total_panels)),
        out_shape=(
            pltpu.VMEM((own_panels, 2, 2 * beams_count - 2), jnp.float32),
            pltpu.VMEM((2, snaps // tile_count), jnp.float32),
        ),
        in_specs=[any_space] * 4,
        out_specs=(vmem, vmem),
        scratch_shapes=[
            pltpu.SMEM(loading.shape, loading.dtype),
            pltpu.VMEM((1, total_panels), jnp.int32),
            pltpu.VMEM(snapshots.shape, snapshots.dtype),
            pltpu.VMEM((tile_count, own_tiles, 2, snaps), snapshots.dtype),
            pltpu.VMEM((own_tiles, beams_count), jnp.int32),
            pltpu.VMEM((tile_count, own_tiles, beams_count), jnp.int32),
            pltpu.VMEM((total_panels, 2 * snaps // LANES, LANES), jnp.float32),
            pltpu.VMEM((own_panels, 2, LANES), jnp.float32),
            dma((6,)),
            dma((tile_count,)),
            dma((tile_count,)),
            dma((tile_count,)),
            dma((tile_count,)),
            dma((devices,)),
            dma((total_panels,)),
            dma((tile_count,)),
            dma((tile_count,)),
        ],
        compiler_params=pltpu.CompilerParams(collective_id=0, has_side_effects=True),
        name="beamformer",
    )(loading, snapshots, beam_codes.T, panel_codes.reshape(1, -1))
    return (jnp.transpose(cancel_t, (0, 2, 1)), beam_out)


def body(mesh_shape, snapshots, beam_codes, panel_codes, loading):
    panel_count, tile_count = mesh_shape
    own_panels, own_tiles, _, snaps = snapshots.shape
    block = snaps // tile_count
    fits = (
        own_panels == tile_count
        and own_tiles % SUBS == 0
        and 4 * beam_codes.shape[0] == LANES
        and (2 * own_panels * panel_count) % SUBS == 0
        and 2 * own_panels * panel_count + 2 <= LANES
        and 2 * snaps == SUBS * LANES
        and block <= LANES
        and LANES % block == 0
    )
    if not fits:
        return plain_body(snapshots, beam_codes, panel_codes, loading)
    return fused_body(panel_count, tile_count, snapshots, beam_codes, panel_codes, loading)


def solution(mesh):
    placed = (P("panel", "tile", None, None), P(None, "tile"), P(), P("panel"))
    return jax.shard_map(
        functools.partial(body, (mesh.shape["panel"], mesh.shape["tile"])),
        mesh=mesh,
        in_specs=placed,
        out_specs=(P("panel", None, None), P(None, "tile")),
        check_vma=False,
    )
```

```python
import functools
import math

import jax
import jax.numpy as jnp
from jax import lax
from jax.experimental import pallas as pl
from jax.experimental.pallas import tpu as pltpu
from jax.sharding import PartitionSpec as P

MESH = pl.DeviceIdType.MESH
LANES = 128
SUBS = 8
WIDE = 2
GRANT = 16 * 1024 * 1024
HIGH = lax.Precision.HIGHEST

phase_levels = 64
array_load = 1.0


def steering_rows(codes, total_tiles):
    angles = codes.astype(jnp.float32) * (2.0 * math.pi / phase_levels)
    cosine = jnp.cos(angles)
    sine = jnp.sin(angles)
    count_beams = codes.shape[0]
    count_tiles = codes.shape[1]
    real_rows = jnp.stack([cosine, sine], axis=-1).reshape(count_beams, 2 * count_tiles)
    imag_rows = jnp.stack([-sine, cosine], axis=-1).reshape(count_beams, 2 * count_tiles)
    table = jnp.stack([real_rows, imag_rows], axis=1).reshape(2 * count_beams, 2 * count_tiles)
    return (table / math.sqrt(total_tiles)).astype(jnp.bfloat16)


def solve_one(factor_one, right_one):
    return jax.scipy.linalg.cho_solve((factor_one, True), right_one)


def cancel_weights(covar):
    factor = jnp.linalg.cholesky(covar[:, 2:, 2:])
    return jax.vmap(solve_one)(factor, covar[:, 2:, :2])


def constraint_matrix(panel_codes):
    angles = panel_codes.astype(jnp.float32) * (2.0 * math.pi / phase_levels)
    cosine = jnp.cos(angles)
    sine = jnp.sin(angles)
    upper = jnp.stack([cosine, -sine], axis=-1)
    lower = jnp.stack([sine, cosine], axis=-1)
    return jnp.stack([upper, lower], axis=1).reshape(2 * panel_codes.shape[0], 2)


def array_weights(covar, constraint):
    factor = jnp.linalg.cholesky(covar)
    solved = jax.scipy.linalg.cho_solve((factor, True), constraint)
    gram = jnp.dot(constraint.T, solved, precision=HIGH)
    determinant = gram[0, 0] * gram[1, 1] - gram[0, 1] * gram[1, 0]
    inverse = (
        jnp.stack([jnp.stack([gram[1, 1], -gram[0, 1]]), jnp.stack([-gram[1, 0], gram[0, 0]])])
        / determinant
    )
    return jnp.dot(solved, inverse, precision=HIGH)


def plain_body(snapshots, beam_codes, panel_codes, loading):
    own_panels, own_tiles, _, snaps = snapshots.shape
    tile_count = lax.axis_size("tile")
    block_snaps = snaps // tile_count
    table = steering_rows(beam_codes, own_tiles * tile_count)
    samples = snapshots.reshape(own_panels, 2 * own_tiles, snaps)
    partial_value = jnp.einsum("bk,pks->pbs", table, samples, preferred_element_type=jnp.float32)
    totals = lax.psum(partial_value, "tile")
    summed = jnp.einsum("pis,pjs->pij", totals, totals, precision=HIGH)
    start = lax.axis_index("tile") * block_snaps
    beams = lax.dynamic_slice_in_dim(totals, start, block_snaps, 2)
    identity = jnp.eye(beams.shape[1], dtype=jnp.float32)
    covar = summed / snaps + loading[:, None, None] * identity[None, :, :]
    cancel = cancel_weights(covar)
    outputs = beams[:, :2, :] - jnp.einsum("pak,pas->pks", cancel, beams[:, 2:, :], precision=HIGH)
    gathered = lax.all_gather(outputs, "panel", axis=0, tiled=True)
    flat = gathered.reshape(gathered.shape[0] * 2, block_snaps)
    array_sum = lax.psum(jnp.dot(flat, flat.T, precision=HIGH), "tile")
    array_covar = array_sum / snaps + array_load * jnp.eye(flat.shape[0], dtype=jnp.float32)
    weights = array_weights(array_covar, constraint_matrix(panel_codes))
    beam_out = jnp.dot(weights.T, flat, precision=HIGH) * math.sqrt(flat.shape[0] // 2)
    return (cancel, beam_out)


def iota(shape, dim):
    return lax.broadcasted_iota(jnp.int32, shape, dim)


def cos_code(code):
    code = code & (phase_levels - 1)
    eighth = phase_levels // 8
    quarter = phase_levels // 4
    quadrant = ((code + eighth) >> 4) & 3
    rest = code - (((code + eighth) >> 4) * quarter)
    x = rest.astype(jnp.float32) * (2.0 * math.pi / phase_levels)
    y = x * x
    cosine = 1.0 + y * (-0.5 + y * (1 / 24 + y * (-1 / 720 + y * (1 / 40320 - y * (1 / 3628800)))))
    sine = x * (1.0 + y * (-1 / 6 + y * (1 / 120 + y * (-1 / 5040 + y * (1 / 362880)))))
    odd = (quadrant & 1) == 1
    flip = jnp.where((quadrant == 1) | (quadrant == 2), -1.0, 1.0)
    return jnp.where(odd, sine, cosine) * flip


def contract(a, b, dims, precision=HIGH):
    return lax.dot_general(a, b, (dims, ((), ())), precision=precision, preferred_element_type=jnp.float32)


def spread(value, row):
    return jnp.broadcast_to(value[row : row + 1], value.shape)


def lane_of(value, where_lane):
    return jnp.take_along_axis(value, jnp.broadcast_to(where_lane, value.shape), axis=1)


def tree(terms):
    terms = list(terms)
    while len(terms) > 1:
        terms = [sum(terms[i : i + 2][1:], terms[i]) for i in range(0, len(terms), 2)]
    return terms[0]


def eliminate(rows, pivots, wide, parts):
    shape = rows[0].shape
    sub, lane = iota(shape, 0), iota(shape, 1)
    span = shape[1] // parts
    first = lane // span * span
    count = len(rows)
    rows = list(rows)

    def pick(value, c):
        if parts > 1:
            return lane_of(value, first + c)
        return jnp.broadcast_to(jnp.sum(jnp.where(lane == c, value, 0.0), axis=1, keepdims=True), shape)

    for base in range(0, count, wide):
        cols = list(range(base * SUBS, min((base + wide) * SUBS, pivots)))
        outer = [(base + wide + k) % count for k in range(count - wide)]
        inner = rows[base : base + wide]
        diag = {c: [pick(value, c) for value in inner] for c in cols}
        factor = {c: [pick(rows[g], c) for g in outer] for c in cols}
        for c in cols[::2]:
            g, s = c // SUBS - base, c % SUBS
            a, b = spread(diag[c][g], s), spread(diag[c + 1][g], s)
            e, d = spread(diag[c][g], s + 1), spread(diag[c + 1][g], s + 1)
            scale = 1.0 / (a * d - b * e)
            top, bottom = sub == s, sub == s + 1
            left = [x * d - y * e for x, y in zip(diag[c], diag[c + 1])]
            right = [y * a - x * b for x, y in zip(diag[c], diag[c + 1])]
            left[g] = jnp.where(top, -d, jnp.where(bottom, e, left[g]))
            right[g] = jnp.where(top, b, jnp.where(bottom, -a, right[g]))
            left = [value * scale for value in left]
            right = [value * scale for value in right]

            def reduce(values):
                row0, row1 = spread(values[g], s), spread(values[g], s + 1)
                kept = list(values)
                kept[g] = jnp.where(top | bottom, 0.0, kept[g])
                return [v - l * row0 - r * row1 for v, l, r in zip(kept, left, right)]

            for k in cols:
                if k > c + 1:
                    diag[k] = reduce(diag[k])
            inner = reduce(inner)
        rows[base : base + wide] = inner
        pivot = {c: spread(inner[c // SUBS - base], c % SUBS) for c in cols}
        for q, g in enumerate(outer):
            rows[g] = rows[g] - tree(factor[c][q] * pivot[c] for c in cols)
    return rows


def gather_kernel(
    sizes, loading_in, snaps_in, codes_in, panel_codes_in, flat, cancels, steer,
    loading, panel_codes, own, got, codes_own, codes_got,
    local_sem, send_a, recv_a, send_c, recv_c, send_f, recv_f, send_w, recv_w,
):
    panel_count, tile_count, total_panels = sizes
    own_panels, own_tiles, _, snaps = snaps_in.shape
    total_tiles = own_tiles * tile_count
    beams_count = codes_in.shape[1]
    width = 2 * beams_count
    chunks = snaps // LANES
    owners = tile_count // 2
    pi, ti = lax.axis_index("panel"), lax.axis_index("tile")
    spare = tile_count - 4
    row = jnp.where(ti == spare, owners - 1, lax.div(ti, 2))
    seat = lambda q: jnp.where(q < owners - 1, 2 * q + 1, spare)
    owner = ti == seat(row)
    mates = [jnp.where(k >= ti, k + 1, k) for k in range(tile_count - 1)]
    panels = [jnp.where(k >= pi, k + 1, k) for k in range(panel_count - 1)]
    seats = []
    for k in range(owners):
        last = (k + owners - 1) % owners
        right = jnp.where(ti < tile_count - 2, k, last)
        seats.append(jnp.where(ti < tile_count // 2, owners - 1 - k, right))

    barrier = pltpu.get_barrier_semaphore()

    @pl.when(owner)
    def _():
        for t in mates:
            pl.semaphore_signal(barrier, inc=1, device_id=(pi, t), device_id_type=MESH)

    for p in panels:
        pl.semaphore_signal(barrier, inc=1, device_id=(p, ti), device_id_type=MESH)
    loads = [
        pltpu.make_async_copy(source, target, local_sem.at[index])
        for index, (source, target) in enumerate((
            (snaps_in, own),
            (codes_in, codes_own),
            (loading_in, loading),
            (panel_codes_in, panel_codes),
        ))
    ]
    for load in loads:
        load.start()
    for load in loads[:2]:
        load.wait()
    pl.semaphore_wait(barrier, panel_count - 1 + owners - jnp.where(owner, 1, 0))

    def code_to(q):
        return pltpu.make_async_remote_copy(
            codes_own, codes_got.at[ti], send_c, recv_c, device_id=(pi, seat(q)), device_id_type=MESH
        )

    def bulk_to(q):
        return pltpu.make_async_remote_copy(
            own.at[pl.ds(2 * q, 2)], got.at[ti], send_a, recv_a,
            device_id=(pi, seat(q)), device_id_type=MESH,
        )

    for q in seats:
        pl.when(seat(q) != ti)(code_to(q).start)
    for q in seats:
        pl.when(seat(q) != ti)(bulk_to(q).start)

    for load in loads[2:]:
        load.wait()
    order = 2 * total_panels
    quarter = phase_levels // 4
    code_row = jnp.broadcast_to(panel_codes[...], (order, total_panels))
    own_code = jnp.where(iota((order, total_panels), 1) == lax.rem(iota((order, total_panels), 0), total_panels), code_row, 0)
    code_col = jnp.broadcast_to(jnp.sum(own_code, axis=1, keepdims=True), (order, LANES))
    lower = iota((order, LANES), 0) >= total_panels
    steer[0] = cos_code(code_col + jnp.where(lower, -quarter, 0))
    steer[1] = cos_code(code_col + jnp.where(lower, 0, quarter))

    mine = pi * own_panels + 2 * row
    me = pi * owners + row
    span = 2 * panel_count
    rank = lax.div(ti, 2) * span + 2 * pi + lax.rem(ti, 2)
    targets = []
    for k in range(panel_count * tile_count - 1):
        n = jnp.where(k >= rank, k + 1, k)
        within = lax.rem(n, span)
        targets.append((lax.div(within, 2), 2 * lax.div(n, span) + lax.rem(within, 2)))

    def flat_to(to):
        return pltpu.make_async_remote_copy(
            flat.at[pl.ds(mine, 2)], flat.at[pl.ds(mine, 2)], send_f, recv_f,
            device_id=to, device_id_type=MESH,
        )

    def cancel_to(t):
        return pltpu.make_async_remote_copy(
            cancels.at[pl.ds(2 * row, 2)], cancels.at[pl.ds(2 * row, 2)], send_w, recv_w,
            device_id=(pi, t), device_id_type=MESH,
        )

    def total_of(ref, count, send, recv):
        part = ref if count == ref.shape[0] else ref.at[pl.ds(0, count)]
        return pltpu.make_async_remote_copy(part, part, send, recv, device_id=(pi, mates[0]), device_id_type=MESH)

    def arrived(ref, count, send, recv):
        total_of(ref, count, send, recv).wait_recv()

    def left_here(ref, count, send, recv):
        while count:
            now = min(count, ref.shape[0])
            total_of(ref, now, send, recv).wait_send()
            count -= now

    @pl.when(owner)
    def _():
        arrived(codes_got, tile_count - 1, send_c, recv_c)
        codes_got[ti] = codes_own[...]
        codes_all = codes_got[...].reshape(total_tiles, beams_count).astype(jnp.float32).astype(jnp.bfloat16)
        beam_of = lax.rem(iota((width, beams_count), 0) + 2, width) >> 1
        b_rows = (beam_of == iota((width, beams_count), 1)).astype(jnp.float32).astype(jnp.bfloat16)
        k_cols = (iota((total_tiles, 2 * total_tiles), 1) >> 1) == iota((total_tiles, 2 * total_tiles), 0)
        tall = contract(b_rows, codes_all, ((1,), (1,)), None)
        wide = contract(tall.astype(jnp.bfloat16), k_cols.astype(jnp.float32).astype(jnp.bfloat16), ((1,), (0,)), None)
        code = (wide + 0.5).astype(jnp.int32)
        turn = (iota(code.shape, 0) & 1) - (iota(code.shape, 1) & 1)
        table = (cos_code(code + quarter * turn) / math.sqrt(total_tiles)).astype(jnp.bfloat16)

        got[ti] = own[pl.ds(2 * row, 2)]
        arrived(got, tile_count - 1, send_a, recv_a)
        beams = [
            contract(table, got[:, h].reshape(2 * total_tiles, snaps), ((1,), (0,)), None) for h in range(2)
        ]
        both = jnp.concatenate(beams, axis=0)
        covar = contract(both, both, ((1,), (1,)))
        square = (width, LANES)
        lane, r_of = iota(square, 1), iota(square, 0)
        left = lane < width
        full = jnp.where(left, covar[:width], covar[width:]) / snaps
        load_lane = jnp.where(left, loading[2 * row], loading[2 * row + 1])
        full = full + jnp.where(lax.rem(lane, width) == r_of, load_lane, 0.0)
        groups = eliminate([full[r : r + SUBS] for r in range(0, width, SUBS)], width - 2, WIDE, 2)
        turned = jnp.concatenate(groups, axis=0).T
        for h in range(2):
            cancels[2 * row + h] = turned[(h + 1) * width - 2 : (h + 1) * width, : width - 2]
        sub, lanes = iota((SUBS, LANES), 0), iota((SUBS, LANES), 1)
        for h in range(2):
            weigh = []
            for k in range(2):
                cols = [-lane_of(value, jnp.full((SUBS, LANES), h * width + width - 2 + k, jnp.int32)) for value in groups]
                cols[-1] = jnp.where(sub < SUBS - 2, cols[-1], jnp.where(sub == SUBS - 2 + k, 1.0, 0.0))
                weigh.append(cols)
            placed = jnp.zeros((SUBS, LANES), jnp.float32)
            for j in range(chunks):
                for k in range(2):
                    total = tree(
                        weigh[k][g] * beams[h][g * SUBS : (g + 1) * SUBS, j * LANES : (j + 1) * LANES]
                        for g in range(width // SUBS)
                    )
                    line = jnp.broadcast_to(jnp.sum(total, axis=0, keepdims=True), (SUBS, LANES))
                    placed = jnp.where(sub == 2 * j + k, line, placed)
            flat[mine + h] = placed
        for to in targets[:2]:
            flat_to(to).start()
        for t in mates:
            cancel_to(t).start()
        for to in targets[2:]:
            flat_to(to).start()

    @pl.when(owner)
    def _():
        arrived(flat, total_panels - 2, send_f, recv_f)
        arrived(cancels, own_panels - 2, send_w, recv_w)
        left_here(codes_got, owners - 1, send_c, recv_c)
        left_here(got, owners - 1, send_a, recv_a)
        left_here(flat, 2 * len(targets), send_f, recv_f)
        left_here(cancels, 2 * len(mates), send_w, recv_w)

    @pl.when(jnp.logical_not(owner))
    def _():
        arrived(flat, total_panels, send_f, recv_f)
        arrived(cancels, own_panels, send_w, recv_w)
        left_here(codes_got, owners, send_c, recv_c)
        left_here(got, owners, send_a, recv_a)


def array_kernel(sizes, flat, cancels, steer, cancel_out, beam_out, out_sem):
    tile_count, total_panels, snaps = sizes
    order = 2 * total_panels
    chunks = snaps // LANES
    count = order // SUBS
    ti = lax.axis_index("tile")
    store = pltpu.make_async_copy(cancels, cancel_out, out_sem)
    store.start()
    parts = [jnp.concatenate([flat[:, 2 * j, :], flat[:, 2 * j + 1, :]], axis=0) for j in range(chunks)]
    joined = jnp.concatenate(parts, axis=1)
    square = (order, LANES)
    lane, r_of = iota(square, 1), iota(square, 0)
    covar = contract(joined, joined, ((1,), (1,))) / snaps
    covar = covar + jnp.where(iota((order, order), 0) == iota((order, order), 1), array_load, 0.0)
    full = jnp.concatenate([covar, jnp.zeros((order, LANES - order), jnp.float32)], axis=1)
    full = jnp.where(lane == order, steer[0], jnp.where(lane == order + 1, steer[1], full))
    block = snaps // tile_count
    per = LANES // block
    chunk, spot = lax.div(ti, per), lax.rem(ti, per)
    mine = parts[0]
    for j in range(1, chunks):
        mine = jnp.where(chunk == j, parts[j], mine)
    turned = mine
    for j in range(1, per):
        turned = jnp.where(spot == j, pltpu.roll(mine, LANES - j * block, 1), turned)
    groups = eliminate([full[r : r + SUBS] for r in range(0, order, SUBS)], order, WIDE, 1)
    solved = [[lane_of(value, jnp.full((SUBS, LANES), order + k, jnp.int32)) for value in groups] for k in range(2)]
    cut = lambda value, g: value[g * SUBS : (g + 1) * SUBS]
    inner = lambda cols, value: jnp.sum(tree(cols[g] * cut(value, g) for g in range(count)), axis=0, keepdims=True)
    s0, s1 = inner(solved[0], turned), inner(solved[1], turned)
    g00, g01 = inner(solved[0], steer[0]), inner(solved[1], steer[0])
    g10, g11 = inner(solved[0], steer[1]), inner(solved[1], steer[1])
    scale = math.sqrt(total_panels) / (g00 * g11 - g01 * g10)
    beam_out[0:1, :] = ((g11 * s0 - g10 * s1) * scale)[:, :block]
    beam_out[1:2, :] = ((g00 * s1 - g01 * s0) * scale)[:, :block]
    store.wait()


def fused_body(panel_count, tile_count, snapshots, beam_codes, panel_codes, loading):
    own_panels, own_tiles, _, snaps = snapshots.shape
    beams_count = beam_codes.shape[0]
    total_panels = own_panels * panel_count
    owners = tile_count // 2
    dma = pltpu.SemaphoreType.DMA
    any_space = pl.BlockSpec(memory_space=pl.ANY)
    vmem = pl.BlockSpec(memory_space=pltpu.VMEM)
    aux = 2 * beams_count - 2
    flat, cancels, steer = pl.pallas_call(
        functools.partial(gather_kernel, (panel_count, tile_count, total_panels)),
        out_shape=(
            pltpu.VMEM((total_panels, 2 * snaps // LANES, LANES), jnp.float32),
            pltpu.VMEM((own_panels, 2, aux), jnp.float32),
            pltpu.VMEM((2, 2 * total_panels, LANES), jnp.float32),
        ),
        in_specs=[any_space] * 4,
        out_specs=(vmem, vmem, vmem),
        scratch_shapes=[
            pltpu.SMEM(loading.shape, loading.dtype),
            pltpu.VMEM((1, total_panels), jnp.int32),
            pltpu.VMEM(snapshots.shape, snapshots.dtype),
            pltpu.VMEM((tile_count, 2, own_tiles, 2, snaps), snapshots.dtype),
            pltpu.VMEM((own_tiles, beams_count), jnp.int32),
            pltpu.VMEM((tile_count, own_tiles, beams_count), jnp.int32),
            dma((4,)),
            dma,
            dma,
            dma,
            dma,
            dma,
            dma,
            dma,
            dma,
        ],
        compiler_params=pltpu.CompilerParams(collective_id=0, has_side_effects=True),
        name="panels",
    )(loading, snapshots, beam_codes.T, panel_codes.reshape(1, -1))
    cancel_t, beam_out = pl.pallas_call(
        functools.partial(array_kernel, (tile_count, total_panels, snaps)),
        out_shape=(
            jax.ShapeDtypeStruct((own_panels, 2, aux), jnp.float32),
            jax.ShapeDtypeStruct((2, snaps // tile_count), jnp.float32),
        ),
        in_specs=[vmem] * 3,
        out_specs=(any_space, vmem),
        scratch_shapes=[dma],
        compiler_params=pltpu.CompilerParams(vmem_limit_bytes=GRANT),
        name="array",
    )(flat, cancels, steer)
    return (jnp.transpose(cancel_t, (0, 2, 1)), beam_out)


def body(mesh_shape, snapshots, beam_codes, panel_codes, loading):
    panel_count, tile_count = mesh_shape
    own_panels, own_tiles, _, snaps = snapshots.shape
    block = snaps // tile_count
    fits = (
        own_panels == tile_count
        and tile_count % 2 == 0
        and tile_count >= 4
        and own_tiles % SUBS == 0
        and 4 * beam_codes.shape[0] == LANES
        and (2 * own_panels * panel_count) % (WIDE * SUBS) == 0
        and 2 * own_panels * panel_count + 2 <= LANES
        and 2 * snaps == SUBS * LANES
        and block <= LANES
        and LANES % block == 0
    )
    if not fits:
        return plain_body(snapshots, beam_codes, panel_codes, loading)
    return fused_body(panel_count, tile_count, snapshots, beam_codes, panel_codes, loading)


def solution(mesh):
    placed = (P("panel", "tile", None, None), P(None, "tile"), P(), P("panel"))
    return jax.shard_map(
        functools.partial(body, (mesh.shape["panel"], mesh.shape["tile"])),
        mesh=mesh,
        in_specs=placed,
        out_specs=(P("panel", None, None), P(None, "tile")),
        check_vma=False,
    )
```

```python
import functools
import math

import jax
import jax.numpy as jnp
from jax import lax
from jax.experimental import pallas as pl
from jax.experimental.pallas import tpu as pltpu
from jax.sharding import PartitionSpec as P

MESH = pl.DeviceIdType.MESH
LANES = 128
SUBS = 8
WIDE = 2
GRANT = 16 * 1024 * 1024
HIGH = lax.Precision.HIGHEST

phase_levels = 64
array_load = 1.0


def steering_rows(codes, total_tiles):
    angles = codes.astype(jnp.float32) * (2.0 * math.pi / phase_levels)
    cosine = jnp.cos(angles)
    sine = jnp.sin(angles)
    count_beams = codes.shape[0]
    count_tiles = codes.shape[1]
    real_rows = jnp.stack([cosine, sine], axis=-1).reshape(count_beams, 2 * count_tiles)
    imag_rows = jnp.stack([-sine, cosine], axis=-1).reshape(count_beams, 2 * count_tiles)
    table = jnp.stack([real_rows, imag_rows], axis=1).reshape(2 * count_beams, 2 * count_tiles)
    return (table / math.sqrt(total_tiles)).astype(jnp.bfloat16)


def solve_one(factor_one, right_one):
    return jax.scipy.linalg.cho_solve((factor_one, True), right_one)


def cancel_weights(covar):
    factor = jnp.linalg.cholesky(covar[:, 2:, 2:])
    return jax.vmap(solve_one)(factor, covar[:, 2:, :2])


def constraint_matrix(panel_codes):
    angles = panel_codes.astype(jnp.float32) * (2.0 * math.pi / phase_levels)
    cosine = jnp.cos(angles)
    sine = jnp.sin(angles)
    upper = jnp.stack([cosine, -sine], axis=-1)
    lower = jnp.stack([sine, cosine], axis=-1)
    return jnp.stack([upper, lower], axis=1).reshape(2 * panel_codes.shape[0], 2)


def array_weights(covar, constraint):
    factor = jnp.linalg.cholesky(covar)
    solved = jax.scipy.linalg.cho_solve((factor, True), constraint)
    gram = jnp.dot(constraint.T, solved, precision=HIGH)
    determinant = gram[0, 0] * gram[1, 1] - gram[0, 1] * gram[1, 0]
    inverse = (
        jnp.stack([jnp.stack([gram[1, 1], -gram[0, 1]]), jnp.stack([-gram[1, 0], gram[0, 0]])])
        / determinant
    )
    return jnp.dot(solved, inverse, precision=HIGH)


def plain_body(snapshots, beam_codes, panel_codes, loading):
    own_panels, own_tiles, _, snaps = snapshots.shape
    tile_count = lax.axis_size("tile")
    block_snaps = snaps // tile_count
    table = steering_rows(beam_codes, own_tiles * tile_count)
    samples = snapshots.reshape(own_panels, 2 * own_tiles, snaps)
    partial_value = jnp.einsum("bk,pks->pbs", table, samples, preferred_element_type=jnp.float32)
    totals = lax.psum(partial_value, "tile")
    summed = jnp.einsum("pis,pjs->pij", totals, totals, precision=HIGH)
    start = lax.axis_index("tile") * block_snaps
    beams = lax.dynamic_slice_in_dim(totals, start, block_snaps, 2)
    identity = jnp.eye(beams.shape[1], dtype=jnp.float32)
    covar = summed / snaps + loading[:, None, None] * identity[None, :, :]
    cancel = cancel_weights(covar)
    outputs = beams[:, :2, :] - jnp.einsum("pak,pas->pks", cancel, beams[:, 2:, :], precision=HIGH)
    gathered = lax.all_gather(outputs, "panel", axis=0, tiled=True)
    flat = gathered.reshape(gathered.shape[0] * 2, block_snaps)
    array_sum = lax.psum(jnp.dot(flat, flat.T, precision=HIGH), "tile")
    array_covar = array_sum / snaps + array_load * jnp.eye(flat.shape[0], dtype=jnp.float32)
    weights = array_weights(array_covar, constraint_matrix(panel_codes))
    beam_out = jnp.dot(weights.T, flat, precision=HIGH) * math.sqrt(flat.shape[0] // 2)
    return (cancel, beam_out)


def iota(shape, dim):
    return lax.broadcasted_iota(jnp.int32, shape, dim)


def cos_code(code):
    code = code & (phase_levels - 1)
    eighth = phase_levels // 8
    quarter = phase_levels // 4
    quadrant = ((code + eighth) >> 4) & 3
    rest = code - (((code + eighth) >> 4) * quarter)
    x = rest.astype(jnp.float32) * (2.0 * math.pi / phase_levels)
    y = x * x
    cosine = 1.0 + y * (-0.5 + y * (1 / 24 + y * (-1 / 720 + y * (1 / 40320 - y * (1 / 3628800)))))
    sine = x * (1.0 + y * (-1 / 6 + y * (1 / 120 + y * (-1 / 5040 + y * (1 / 362880)))))
    odd = (quadrant & 1) == 1
    flip = jnp.where((quadrant == 1) | (quadrant == 2), -1.0, 1.0)
    return jnp.where(odd, sine, cosine) * flip


def contract(a, b, dims, precision=HIGH):
    return lax.dot_general(a, b, (dims, ((), ())), precision=precision, preferred_element_type=jnp.float32)


def gram(value):
    count = value.shape[0]
    half = jnp.bfloat16
    high = value.astype(half)
    rest = value - high.astype(jnp.float32)
    middle = rest.astype(half)
    low = (rest - middle.astype(jnp.float32)).astype(half)
    across = ((1,), (1,))
    if count % LANES == 0:
        first = contract(jnp.concatenate([high, middle, low], axis=0), jnp.concatenate([high, middle], axis=0), across, None)
        third = contract(high, low, across, None)
        row = lambda k: first[k * count : (k + 1) * count]
        small = row(2)[:, :count] + third + row(1)[:, count:]
        return small + (row(1)[:, :count] + row(0)[:, count:]) + row(0)[:, :count]
    first = contract(jnp.concatenate([high, middle, low], axis=0), high, across, None)
    second = contract(jnp.concatenate([high, middle], axis=0), middle, across, None)
    third = contract(high, low, across, None)
    small = first[2 * count :] + third + second[count:]
    return small + (first[count : 2 * count] + second[:count]) + first[:count]


def spread(value, row):
    return jnp.broadcast_to(value[row : row + 1], value.shape)


def lane_of(value, where_lane):
    return jnp.take_along_axis(value, jnp.broadcast_to(where_lane, value.shape), axis=1)


def tree(terms):
    terms = list(terms)
    while len(terms) > 1:
        terms = [sum(terms[i : i + 2][1:], terms[i]) for i in range(0, len(terms), 2)]
    return terms[0]


def eliminate(rows, pivots, wide, parts):
    shape = rows[0].shape
    sub, lane = iota(shape, 0), iota(shape, 1)
    span = shape[1] // parts
    first = lane // span * span
    count = len(rows)
    rows = list(rows)

    def pick(value, c):
        if parts > 1:
            return lane_of(value, first + c)
        return jnp.broadcast_to(jnp.sum(jnp.where(lane == c, value, 0.0), axis=1, keepdims=True), shape)

    for base in range(0, count, wide):
        cols = list(range(base * SUBS, min((base + wide) * SUBS, pivots)))
        outer = [(base + wide + k) % count for k in range(count - wide)]
        inner = rows[base : base + wide]
        diag = {c: [pick(value, c) for value in inner] for c in cols}
        factor = {c: [pick(rows[g], c) for g in outer] for c in cols}
        for c in cols[::2]:
            g, s = c // SUBS - base, c % SUBS
            a, b = spread(diag[c][g], s), spread(diag[c + 1][g], s)
            e, d = spread(diag[c][g], s + 1), spread(diag[c + 1][g], s + 1)
            scale = 1.0 / (a * d - b * e)
            top, bottom = sub == s, sub == s + 1
            left = [x * d - y * e for x, y in zip(diag[c], diag[c + 1])]
            right = [y * a - x * b for x, y in zip(diag[c], diag[c + 1])]
            left[g] = jnp.where(top, -d, jnp.where(bottom, e, left[g]))
            right[g] = jnp.where(top, b, jnp.where(bottom, -a, right[g]))
            left = [value * scale for value in left]
            right = [value * scale for value in right]

            def reduce(values):
                row0, row1 = spread(values[g], s), spread(values[g], s + 1)
                kept = list(values)
                kept[g] = jnp.where(top | bottom, 0.0, kept[g])
                return [v - l * row0 - r * row1 for v, l, r in zip(kept, left, right)]

            for k in cols:
                if k > c + 1:
                    diag[k] = reduce(diag[k])
            inner = reduce(inner)
        rows[base : base + wide] = inner
        pivot = {c: spread(inner[c // SUBS - base], c % SUBS) for c in cols}
        for q, g in enumerate(outer):
            rows[g] = rows[g] - tree(factor[c][q] * pivot[c] for c in cols)
    return rows


def gather_kernel(
    sizes, loading_in, snaps_in, codes_in, panel_codes_in, flat, cancels, steer,
    loading, panel_codes, own, got, codes_own, codes_got,
    local_sem, send_a, recv_a, send_c, recv_c, send_f, recv_f, send_w, recv_w,
):
    panel_count, tile_count, total_panels = sizes
    own_panels, own_tiles, _, snaps = snaps_in.shape
    total_tiles = own_tiles * tile_count
    beams_count = codes_in.shape[1]
    width = 2 * beams_count
    chunks = snaps // LANES
    owners = tile_count // 2
    pi, ti = lax.axis_index("panel"), lax.axis_index("tile")
    spare = tile_count - 4
    row = jnp.where(ti == spare, owners - 1, lax.div(ti, 2))
    seat = lambda q: jnp.where(q < owners - 1, 2 * q + 1, spare)
    owner = ti == seat(row)
    mates = [jnp.where(k >= ti, k + 1, k) for k in range(tile_count - 1)]
    panels = [jnp.where(k >= pi, k + 1, k) for k in range(panel_count - 1)]
    seats = []
    for k in range(owners):
        last = (k + owners - 1) % owners
        right = jnp.where(ti < tile_count - 2, k, last)
        seats.append(jnp.where(ti < tile_count // 2, owners - 1 - k, right))

    barrier = pltpu.get_barrier_semaphore()

    loads = [
        pltpu.make_async_copy(source, target, local_sem.at[index])
        for index, (source, target) in enumerate((
            (codes_in, codes_own),
            (loading_in, loading),
            (panel_codes_in, panel_codes),
        ))
    ]
    parts = [pltpu.make_async_copy(snaps_in, own, local_sem.at[len(loads)])]
    for load in parts + loads:
        load.start()

    @pl.when(owner)
    def _():
        for t in mates:
            pl.semaphore_signal(barrier, inc=1, device_id=(pi, t), device_id_type=MESH)

    for p in panels:
        pl.semaphore_signal(barrier, inc=1, device_id=(p, ti), device_id_type=MESH)
    for load in parts + loads[:1]:
        load.wait()
    pl.semaphore_wait(barrier, panel_count - 1 + owners - jnp.where(owner, 1, 0))

    def code_to(q):
        return pltpu.make_async_remote_copy(
            codes_own, codes_got.at[ti], send_c, recv_c, device_id=(pi, seat(q)), device_id_type=MESH
        )

    def bulk_to(q):
        return pltpu.make_async_remote_copy(
            own.at[pl.ds(2 * q, 2)], got.at[ti], send_a, recv_a,
            device_id=(pi, seat(q)), device_id_type=MESH,
        )

    for q in seats:
        pl.when(seat(q) != ti)(code_to(q).start)
    for q in seats:
        pl.when(seat(q) != ti)(bulk_to(q).start)

    for load in loads[1:]:
        load.wait()
    order = 2 * total_panels
    quarter = phase_levels // 4
    code_row = jnp.broadcast_to(panel_codes[...], (order, total_panels))
    own_code = jnp.where(iota((order, total_panels), 1) == lax.rem(iota((order, total_panels), 0), total_panels), code_row, 0)
    code_col = jnp.broadcast_to(jnp.sum(own_code, axis=1, keepdims=True), (order, LANES))
    lower = iota((order, LANES), 0) >= total_panels
    steer[0] = cos_code(code_col + jnp.where(lower, -quarter, 0))
    steer[1] = cos_code(code_col + jnp.where(lower, 0, quarter))

    mine = pi * own_panels + 2 * row
    me = pi * owners + row
    span = 2 * panel_count
    rank = lax.div(ti, 2) * span + 2 * pi + lax.rem(ti, 2)
    targets = []
    for k in range(panel_count * tile_count - 1):
        n = jnp.where(k >= rank, k + 1, k)
        within = lax.rem(n, span)
        targets.append((lax.div(within, 2), 2 * lax.div(n, span) + lax.rem(within, 2)))

    def flat_to(to):
        return pltpu.make_async_remote_copy(
            flat.at[pl.ds(mine, 2)], flat.at[pl.ds(mine, 2)], send_f, recv_f,
            device_id=to, device_id_type=MESH,
        )

    def cancel_to(t):
        return pltpu.make_async_remote_copy(
            cancels.at[pl.ds(2 * row, 2)], cancels.at[pl.ds(2 * row, 2)], send_w, recv_w,
            device_id=(pi, t), device_id_type=MESH,
        )

    def total_of(ref, count, send, recv):
        part = ref if count == ref.shape[0] else ref.at[pl.ds(0, count)]
        return pltpu.make_async_remote_copy(part, part, send, recv, device_id=(pi, mates[0]), device_id_type=MESH)

    def arrived(ref, count, send, recv):
        total_of(ref, count, send, recv).wait_recv()

    def left_here(ref, count, send, recv):
        while count:
            now = min(count, ref.shape[0])
            total_of(ref, now, send, recv).wait_send()
            count -= now

    @pl.when(owner)
    def _():
        arrived(codes_got, tile_count - 1, send_c, recv_c)
        codes_got[ti] = codes_own[...]
        codes_all = codes_got[...].reshape(total_tiles, beams_count).astype(jnp.float32).astype(jnp.bfloat16)
        beam_of = lax.rem(iota((width, beams_count), 0) + 2, width) >> 1
        b_rows = (beam_of == iota((width, beams_count), 1)).astype(jnp.float32).astype(jnp.bfloat16)
        k_cols = (iota((total_tiles, 2 * total_tiles), 1) >> 1) == iota((total_tiles, 2 * total_tiles), 0)
        tall = contract(b_rows, codes_all, ((1,), (1,)), None)
        wide = contract(tall.astype(jnp.bfloat16), k_cols.astype(jnp.float32).astype(jnp.bfloat16), ((1,), (0,)), None)
        code = (wide + 0.5).astype(jnp.int32)
        turn = (iota(code.shape, 0) & 1) - (iota(code.shape, 1) & 1)
        table = (cos_code(code + quarter * turn) / math.sqrt(total_tiles)).astype(jnp.bfloat16)

        got[ti] = own[pl.ds(2 * row, 2)]
        arrived(got, tile_count - 1, send_a, recv_a)
        beams = [
            contract(table, got[:, h].reshape(2 * total_tiles, snaps), ((1,), (0,)), None) for h in range(2)
        ]
        both = jnp.concatenate(beams, axis=0)
        covar = gram(both)
        square = (width, LANES)
        lane, r_of = iota(square, 1), iota(square, 0)
        left = lane < width
        full = jnp.where(left, covar[:width], covar[width:]) / snaps
        load_lane = jnp.where(left, loading[2 * row], loading[2 * row + 1])
        full = full + jnp.where(lax.rem(lane, width) == r_of, load_lane, 0.0)
        groups = eliminate([full[r : r + SUBS] for r in range(0, width, SUBS)], width - 2, WIDE, 2)
        turned = jnp.concatenate(groups, axis=0).T
        for h in range(2):
            cancels[2 * row + h] = turned[(h + 1) * width - 2 : (h + 1) * width, : width - 2]
        sub, lanes = iota((SUBS, LANES), 0), iota((SUBS, LANES), 1)
        for h in range(2):
            weigh = []
            for k in range(2):
                cols = [-lane_of(value, jnp.full((SUBS, LANES), h * width + width - 2 + k, jnp.int32)) for value in groups]
                cols[-1] = jnp.where(sub < SUBS - 2, cols[-1], jnp.where(sub == SUBS - 2 + k, 1.0, 0.0))
                weigh.append(cols)
            placed = jnp.zeros((SUBS, LANES), jnp.float32)
            for j in range(chunks):
                for k in range(2):
                    total = tree(
                        weigh[k][g] * beams[h][g * SUBS : (g + 1) * SUBS, j * LANES : (j + 1) * LANES]
                        for g in range(width // SUBS)
                    )
                    line = jnp.broadcast_to(jnp.sum(total, axis=0, keepdims=True), (SUBS, LANES))
                    placed = jnp.where(sub == 2 * j + k, line, placed)
            flat[mine + h] = placed
        for to in targets[:2]:
            flat_to(to).start()
        for t in mates:
            cancel_to(t).start()
        for to in targets[2:]:
            flat_to(to).start()

    @pl.when(owner)
    def _():
        arrived(flat, total_panels - 2, send_f, recv_f)
        arrived(cancels, own_panels - 2, send_w, recv_w)
        left_here(codes_got, owners - 1, send_c, recv_c)
        left_here(got, owners - 1, send_a, recv_a)
        left_here(flat, 2 * len(targets), send_f, recv_f)
        left_here(cancels, 2 * len(mates), send_w, recv_w)

    @pl.when(jnp.logical_not(owner))
    def _():
        arrived(flat, total_panels, send_f, recv_f)
        arrived(cancels, own_panels, send_w, recv_w)
        left_here(codes_got, owners, send_c, recv_c)
        left_here(got, owners, send_a, recv_a)


def array_kernel(sizes, flat, cancels, steer, cancel_out, beam_out, out_sem):
    tile_count, total_panels, snaps = sizes
    order = 2 * total_panels
    chunks = snaps // LANES
    count = order // SUBS
    ti = lax.axis_index("tile")
    store = pltpu.make_async_copy(cancels, cancel_out, out_sem)
    store.start()
    parts = [jnp.concatenate([flat[:, 2 * j, :], flat[:, 2 * j + 1, :]], axis=0) for j in range(chunks)]
    joined = jnp.concatenate(parts, axis=1)
    square = (order, LANES)
    lane, r_of = iota(square, 1), iota(square, 0)
    covar = gram(joined) / snaps
    covar = covar + jnp.where(iota((order, order), 0) == iota((order, order), 1), array_load, 0.0)
    full = jnp.concatenate([covar, jnp.zeros((order, LANES - order), jnp.float32)], axis=1)
    full = jnp.where(lane == order, steer[0], jnp.where(lane == order + 1, steer[1], full))
    block = snaps // tile_count
    per = LANES // block
    chunk, spot = lax.div(ti, per), lax.rem(ti, per)
    mine = parts[0]
    for j in range(1, chunks):
        mine = jnp.where(chunk == j, parts[j], mine)
    turned = mine
    for j in range(1, per):
        turned = jnp.where(spot == j, pltpu.roll(mine, LANES - j * block, 1), turned)
    groups = eliminate([full[r : r + SUBS] for r in range(0, order, SUBS)], order, WIDE, 1)
    solved = [[lane_of(value, jnp.full((SUBS, LANES), order + k, jnp.int32)) for value in groups] for k in range(2)]
    cut = lambda value, g: value[g * SUBS : (g + 1) * SUBS]
    inner = lambda cols, value: jnp.sum(tree(cols[g] * cut(value, g) for g in range(count)), axis=0, keepdims=True)
    s0, s1 = inner(solved[0], turned), inner(solved[1], turned)
    g00, g01 = inner(solved[0], steer[0]), inner(solved[1], steer[0])
    g10, g11 = inner(solved[0], steer[1]), inner(solved[1], steer[1])
    scale = math.sqrt(total_panels) / (g00 * g11 - g01 * g10)
    beam_out[0:1, :] = ((g11 * s0 - g10 * s1) * scale)[:, :block]
    beam_out[1:2, :] = ((g00 * s1 - g01 * s0) * scale)[:, :block]
    store.wait()


def fused_body(panel_count, tile_count, snapshots, beam_codes, panel_codes, loading):
    own_panels, own_tiles, _, snaps = snapshots.shape
    beams_count = beam_codes.shape[0]
    total_panels = own_panels * panel_count
    owners = tile_count // 2
    dma = pltpu.SemaphoreType.DMA
    any_space = pl.BlockSpec(memory_space=pl.ANY)
    vmem = pl.BlockSpec(memory_space=pltpu.VMEM)
    aux = 2 * beams_count - 2
    flat, cancels, steer = pl.pallas_call(
        functools.partial(gather_kernel, (panel_count, tile_count, total_panels)),
        out_shape=(
            pltpu.VMEM((total_panels, 2 * snaps // LANES, LANES), jnp.float32),
            pltpu.VMEM((own_panels, 2, aux), jnp.float32),
            pltpu.VMEM((2, 2 * total_panels, LANES), jnp.float32),
        ),
        in_specs=[any_space] * 4,
        out_specs=(vmem, vmem, vmem),
        scratch_shapes=[
            pltpu.SMEM(loading.shape, loading.dtype),
            pltpu.VMEM((1, total_panels), jnp.int32),
            pltpu.VMEM(snapshots.shape, snapshots.dtype),
            pltpu.VMEM((tile_count, 2, own_tiles, 2, snaps), snapshots.dtype),
            pltpu.VMEM((own_tiles, beams_count), jnp.int32),
            pltpu.VMEM((tile_count, own_tiles, beams_count), jnp.int32),
            dma((4,)),
            dma,
            dma,
            dma,
            dma,
            dma,
            dma,
            dma,
            dma,
        ],
        compiler_params=pltpu.CompilerParams(collective_id=0, has_side_effects=True),
        name="panels",
    )(loading, snapshots, beam_codes.T, panel_codes.reshape(1, -1))
    cancel_t, beam_out = pl.pallas_call(
        functools.partial(array_kernel, (tile_count, total_panels, snaps)),
        out_shape=(
            jax.ShapeDtypeStruct((own_panels, 2, aux), jnp.float32),
            jax.ShapeDtypeStruct((2, snaps // tile_count), jnp.float32),
        ),
        in_specs=[vmem] * 3,
        out_specs=(any_space, vmem),
        scratch_shapes=[dma],
        compiler_params=pltpu.CompilerParams(vmem_limit_bytes=GRANT),
        name="array",
    )(flat, cancels, steer)
    return (jnp.transpose(cancel_t, (0, 2, 1)), beam_out)


def body(mesh_shape, snapshots, beam_codes, panel_codes, loading):
    panel_count, tile_count = mesh_shape
    own_panels, own_tiles, _, snaps = snapshots.shape
    block = snaps // tile_count
    fits = (
        own_panels == tile_count
        and tile_count % 2 == 0
        and tile_count >= 4
        and own_tiles % SUBS == 0
        and 4 * beam_codes.shape[0] == LANES
        and (2 * own_panels * panel_count) % (WIDE * SUBS) == 0
        and 2 * own_panels * panel_count + 2 <= LANES
        and 2 * snaps == SUBS * LANES
        and block <= LANES
        and LANES % block == 0
    )
    if not fits:
        return plain_body(snapshots, beam_codes, panel_codes, loading)
    return fused_body(panel_count, tile_count, snapshots, beam_codes, panel_codes, loading)


def solution(mesh):
    placed = (P("panel", "tile", None, None), P(None, "tile"), P(), P("panel"))
    return jax.shard_map(
        functools.partial(body, (mesh.shape["panel"], mesh.shape["tile"])),
        mesh=mesh,
        in_specs=placed,
        out_specs=(P("panel", None, None), P(None, "tile")),
        check_vma=False,
    )
```

```python
import functools
import math

import jax
import jax.numpy as jnp
from jax import lax
from jax.experimental import pallas as pl
from jax.experimental.pallas import tpu as pltpu
from jax.sharding import PartitionSpec as P

MESH = pl.DeviceIdType.MESH
LANES = 128
SUBS = 8
WIDE = 2
GRANT = 16 * 1024 * 1024
HIGH = lax.Precision.HIGHEST

phase_levels = 64
array_load = 1.0


def steering_rows(codes, total_tiles):
    angles = codes.astype(jnp.float32) * (2.0 * math.pi / phase_levels)
    cosine = jnp.cos(angles)
    sine = jnp.sin(angles)
    count_beams = codes.shape[0]
    count_tiles = codes.shape[1]
    real_rows = jnp.stack([cosine, sine], axis=-1).reshape(count_beams, 2 * count_tiles)
    imag_rows = jnp.stack([-sine, cosine], axis=-1).reshape(count_beams, 2 * count_tiles)
    table = jnp.stack([real_rows, imag_rows], axis=1).reshape(2 * count_beams, 2 * count_tiles)
    return (table / math.sqrt(total_tiles)).astype(jnp.bfloat16)


def solve_one(factor_one, right_one):
    return jax.scipy.linalg.cho_solve((factor_one, True), right_one)


def cancel_weights(covar):
    factor = jnp.linalg.cholesky(covar[:, 2:, 2:])
    return jax.vmap(solve_one)(factor, covar[:, 2:, :2])


def constraint_matrix(panel_codes):
    angles = panel_codes.astype(jnp.float32) * (2.0 * math.pi / phase_levels)
    cosine = jnp.cos(angles)
    sine = jnp.sin(angles)
    upper = jnp.stack([cosine, -sine], axis=-1)
    lower = jnp.stack([sine, cosine], axis=-1)
    return jnp.stack([upper, lower], axis=1).reshape(2 * panel_codes.shape[0], 2)


def array_weights(covar, constraint):
    factor = jnp.linalg.cholesky(covar)
    solved = jax.scipy.linalg.cho_solve((factor, True), constraint)
    gram = jnp.dot(constraint.T, solved, precision=HIGH)
    determinant = gram[0, 0] * gram[1, 1] - gram[0, 1] * gram[1, 0]
    inverse = (
        jnp.stack([jnp.stack([gram[1, 1], -gram[0, 1]]), jnp.stack([-gram[1, 0], gram[0, 0]])])
        / determinant
    )
    return jnp.dot(solved, inverse, precision=HIGH)


def plain_body(snapshots, beam_codes, panel_codes, loading):
    own_panels, own_tiles, _, snaps = snapshots.shape
    tile_count = lax.axis_size("tile")
    block_snaps = snaps // tile_count
    table = steering_rows(beam_codes, own_tiles * tile_count)
    samples = snapshots.reshape(own_panels, 2 * own_tiles, snaps)
    partial_value = jnp.einsum("bk,pks->pbs", table, samples, preferred_element_type=jnp.float32)
    totals = lax.psum(partial_value, "tile")
    summed = jnp.einsum("pis,pjs->pij", totals, totals, precision=HIGH)
    start = lax.axis_index("tile") * block_snaps
    beams = lax.dynamic_slice_in_dim(totals, start, block_snaps, 2)
    identity = jnp.eye(beams.shape[1], dtype=jnp.float32)
    covar = summed / snaps + loading[:, None, None] * identity[None, :, :]
    cancel = cancel_weights(covar)
    outputs = beams[:, :2, :] - jnp.einsum("pak,pas->pks", cancel, beams[:, 2:, :], precision=HIGH)
    gathered = lax.all_gather(outputs, "panel", axis=0, tiled=True)
    flat = gathered.reshape(gathered.shape[0] * 2, block_snaps)
    array_sum = lax.psum(jnp.dot(flat, flat.T, precision=HIGH), "tile")
    array_covar = array_sum / snaps + array_load * jnp.eye(flat.shape[0], dtype=jnp.float32)
    weights = array_weights(array_covar, constraint_matrix(panel_codes))
    beam_out = jnp.dot(weights.T, flat, precision=HIGH) * math.sqrt(flat.shape[0] // 2)
    return (cancel, beam_out)


def iota(shape, dim):
    return lax.broadcasted_iota(jnp.int32, shape, dim)


def cos_code(code):
    code = code & (phase_levels - 1)
    eighth = phase_levels // 8
    quarter = phase_levels // 4
    quadrant = ((code + eighth) >> 4) & 3
    rest = code - (((code + eighth) >> 4) * quarter)
    x = rest.astype(jnp.float32) * (2.0 * math.pi / phase_levels)
    y = x * x
    cosine = 1.0 + y * (-0.5 + y * (1 / 24 + y * (-1 / 720 + y * (1 / 40320 - y * (1 / 3628800)))))
    sine = x * (1.0 + y * (-1 / 6 + y * (1 / 120 + y * (-1 / 5040 + y * (1 / 362880)))))
    odd = (quadrant & 1) == 1
    flip = jnp.where((quadrant == 1) | (quadrant == 2), -1.0, 1.0)
    return jnp.where(odd, sine, cosine) * flip


def contract(a, b, dims, precision=HIGH):
    return lax.dot_general(a, b, (dims, ((), ())), precision=precision, preferred_element_type=jnp.float32)


def gram(value):
    count = value.shape[0]
    half = jnp.bfloat16
    high = value.astype(half)
    rest = value - high.astype(jnp.float32)
    middle = rest.astype(half)
    low = (rest - middle.astype(jnp.float32)).astype(half)
    across = ((1,), (1,))
    if count % LANES == 0:
        first = contract(jnp.concatenate([high, middle, low], axis=0), jnp.concatenate([high, middle], axis=0), across, None)
        third = contract(high, low, across, None)
        row = lambda k: first[k * count : (k + 1) * count]
        small = row(2)[:, :count] + third + row(1)[:, count:]
        return small + (row(1)[:, :count] + row(0)[:, count:]) + row(0)[:, :count]
    first = contract(jnp.concatenate([high, middle, low], axis=0), high, across, None)
    second = contract(jnp.concatenate([high, middle], axis=0), middle, across, None)
    third = contract(high, low, across, None)
    small = first[2 * count :] + third + second[count:]
    return small + (first[count : 2 * count] + second[:count]) + first[:count]


def spread(value, row):
    return jnp.broadcast_to(value[row : row + 1], value.shape)


def lane_of(value, where_lane):
    return jnp.take_along_axis(value, jnp.broadcast_to(where_lane, value.shape), axis=1)


def tree(terms):
    terms = list(terms)
    while len(terms) > 1:
        terms = [sum(terms[i : i + 2][1:], terms[i]) for i in range(0, len(terms), 2)]
    return terms[0]


def eliminate(rows, pivots, wide, parts, sides=()):
    shape = rows[0].shape
    sub, lane = iota(shape, 0), iota(shape, 1)
    span = shape[1] // parts
    first = lane // span * span
    count = len(rows)
    rows = list(rows)

    def pick(value, c):
        if parts > 1:
            return lane_of(value, first + c)
        return jnp.broadcast_to(jnp.sum(jnp.where(lane == c, value, 0.0), axis=1, keepdims=True), shape)

    for base in range(0, count, wide):
        cols = list(range(base * SUBS, min((base + wide) * SUBS, pivots)))
        outer = [(base + wide + k) % count for k in range(count - wide)]
        inner = rows[base : base + wide]
        diag, factor = {}, {}
        for c in cols:
            diag[c] = [pick(value, c) for value in inner]
            factor[c] = [pick(rows[g], c) for g in outer]
        ending = bool(sides) and base + wide >= count
        if ending:
            rest = {c: [pick(rows[g], c) for g in outer] for c in sides}
            diag.update({c: [pick(value, c) for value in inner] for c in sides})
        for c in cols[::2]:
            g, s = c // SUBS - base, c % SUBS
            a, b = spread(diag[c][g], s), spread(diag[c + 1][g], s)
            e, d = spread(diag[c][g], s + 1), spread(diag[c + 1][g], s + 1)
            scale = 1.0 / (a * d - b * e)
            top, bottom = sub == s, sub == s + 1
            left = [x * d - y * e for x, y in zip(diag[c], diag[c + 1])]
            right = [y * a - x * b for x, y in zip(diag[c], diag[c + 1])]
            left[g] = jnp.where(top, -d, jnp.where(bottom, e, left[g]))
            right[g] = jnp.where(top, b, jnp.where(bottom, -a, right[g]))
            left = [value * scale for value in left]
            right = [value * scale for value in right]

            def reduce(values):
                row0, row1 = spread(values[g], s), spread(values[g], s + 1)
                kept = list(values)
                kept[g] = jnp.where(top | bottom, 0.0, kept[g])
                return [v - l * row0 - r * row1 for v, l, r in zip(kept, left, right)]

            for k in diag:
                if k > c + 1:
                    diag[k] = reduce(diag[k])
            if not ending:
                inner = reduce(inner)
        if ending:
            solved = []
            for k in sides:
                pivot = {c: spread(diag[k][c // SUBS - base], c % SUBS) for c in cols}
                found = {g: rest[k][q] - tree(factor[c][q] * pivot[c] for c in cols) for q, g in enumerate(outer)}
                found.update({base + g: value for g, value in enumerate(diag[k])})
                solved.append([found[g] for g in range(count)])
            return solved
        rows[base : base + wide] = inner
        pivot = {c: spread(inner[c // SUBS - base], c % SUBS) for c in cols}
        for q, g in enumerate(outer):
            rows[g] = rows[g] - tree(factor[c][q] * pivot[c] for c in cols)
    return rows


def gather_kernel(
    sizes, loading_in, snaps_in, codes_in, panel_codes_in, flat, cancels, steer,
    loading, panel_codes, own, got, codes_own, codes_got,
    local_sem, send_a, recv_a, send_c, recv_c, send_f, recv_f, send_w, recv_w,
):
    panel_count, tile_count, total_panels = sizes
    own_panels, own_tiles, _, snaps = snaps_in.shape
    total_tiles = own_tiles * tile_count
    beams_count = codes_in.shape[1]
    width = 2 * beams_count
    chunks = snaps // LANES
    owners = tile_count // 2
    pi, ti = lax.axis_index("panel"), lax.axis_index("tile")
    spare = tile_count - 4
    row = jnp.where(ti == spare, owners - 1, lax.div(ti, 2))
    seat = lambda q: jnp.where(q < owners - 1, 2 * q + 1, spare)
    owner = ti == seat(row)
    mates = [jnp.where(k >= ti, k + 1, k) for k in range(tile_count - 1)]
    panels = [jnp.where(k >= pi, k + 1, k) for k in range(panel_count - 1)]
    seats = []
    for k in range(owners):
        last = (k + owners - 1) % owners
        right = jnp.where(ti < tile_count - 2, k, last)
        seats.append(jnp.where(ti < tile_count // 2, owners - 1 - k, right))

    barrier = pltpu.get_barrier_semaphore()

    loads = [
        pltpu.make_async_copy(source, target, local_sem.at[index])
        for index, (source, target) in enumerate((
            (codes_in, codes_own),
            (loading_in, loading),
            (panel_codes_in, panel_codes),
        ))
    ]
    parts = [pltpu.make_async_copy(snaps_in, own, local_sem.at[len(loads)])]
    for load in parts + loads:
        load.start()

    @pl.when(owner)
    def _():
        for t in mates:
            pl.semaphore_signal(barrier, inc=1, device_id=(pi, t), device_id_type=MESH)

    for p in panels:
        pl.semaphore_signal(barrier, inc=1, device_id=(p, ti), device_id_type=MESH)
    for load in parts + loads[:1]:
        load.wait()
    pl.semaphore_wait(barrier, panel_count - 1 + owners - jnp.where(owner, 1, 0))

    def code_to(q):
        return pltpu.make_async_remote_copy(
            codes_own, codes_got.at[ti], send_c, recv_c, device_id=(pi, seat(q)), device_id_type=MESH
        )

    def bulk_to(q):
        return pltpu.make_async_remote_copy(
            own.at[pl.ds(2 * q, 2)], got.at[ti], send_a, recv_a,
            device_id=(pi, seat(q)), device_id_type=MESH,
        )

    for q in seats:
        pl.when(seat(q) != ti)(code_to(q).start)
    for q in seats:
        pl.when(seat(q) != ti)(bulk_to(q).start)

    for load in loads[1:]:
        load.wait()
    order = 2 * total_panels
    quarter = phase_levels // 4
    code_row = jnp.broadcast_to(panel_codes[...], (order, total_panels))
    own_code = jnp.where(iota((order, total_panels), 1) == lax.rem(iota((order, total_panels), 0), total_panels), code_row, 0)
    code_col = jnp.broadcast_to(jnp.sum(own_code, axis=1, keepdims=True), (order, LANES))
    lower = iota((order, LANES), 0) >= total_panels
    steer[0] = cos_code(code_col + jnp.where(lower, -quarter, 0))
    steer[1] = cos_code(code_col + jnp.where(lower, 0, quarter))

    mine = pi * own_panels + 2 * row
    me = pi * owners + row
    span = 2 * panel_count
    rank = lax.div(ti, 2) * span + 2 * pi + lax.rem(ti, 2)
    targets = []
    for k in range(panel_count * tile_count - 1):
        n = jnp.where(k >= rank, k + 1, k)
        within = lax.rem(n, span)
        targets.append((lax.div(within, 2), 2 * lax.div(n, span) + lax.rem(within, 2)))

    def flat_to(to):
        return pltpu.make_async_remote_copy(
            flat.at[pl.ds(mine, 2)], flat.at[pl.ds(mine, 2)], send_f, recv_f,
            device_id=to, device_id_type=MESH,
        )

    def cancel_to(t):
        return pltpu.make_async_remote_copy(
            cancels.at[pl.ds(2 * row, 2)], cancels.at[pl.ds(2 * row, 2)], send_w, recv_w,
            device_id=(pi, t), device_id_type=MESH,
        )

    def total_of(ref, count, send, recv):
        part = ref if count == ref.shape[0] else ref.at[pl.ds(0, count)]
        return pltpu.make_async_remote_copy(part, part, send, recv, device_id=(pi, mates[0]), device_id_type=MESH)

    def arrived(ref, count, send, recv):
        total_of(ref, count, send, recv).wait_recv()

    def left_here(ref, count, send, recv):
        while count:
            now = min(count, ref.shape[0])
            total_of(ref, now, send, recv).wait_send()
            count -= now

    @pl.when(owner)
    def _():
        arrived(codes_got, tile_count - 1, send_c, recv_c)
        codes_got[ti] = codes_own[...]
        codes_all = codes_got[...].reshape(total_tiles, beams_count).astype(jnp.float32).astype(jnp.bfloat16)
        beam_of = lax.rem(iota((width, beams_count), 0) + 2, width) >> 1
        b_rows = (beam_of == iota((width, beams_count), 1)).astype(jnp.float32).astype(jnp.bfloat16)
        k_cols = (iota((total_tiles, 2 * total_tiles), 1) >> 1) == iota((total_tiles, 2 * total_tiles), 0)
        tall = contract(b_rows, codes_all, ((1,), (1,)), None)
        wide = contract(tall.astype(jnp.bfloat16), k_cols.astype(jnp.float32).astype(jnp.bfloat16), ((1,), (0,)), None)
        code = (wide + 0.5).astype(jnp.int32)
        turn = (iota(code.shape, 0) & 1) - (iota(code.shape, 1) & 1)
        table = (cos_code(code + quarter * turn) / math.sqrt(total_tiles)).astype(jnp.bfloat16)

        got[ti] = own[pl.ds(2 * row, 2)]
        arrived(got, tile_count - 1, send_a, recv_a)
        beams = [
            contract(table, got[:, h].reshape(2 * total_tiles, snaps), ((1,), (0,)), None) for h in range(2)
        ]
        both = jnp.concatenate(beams, axis=0)
        covar = gram(both)
        square = (width, LANES)
        lane, r_of = iota(square, 1), iota(square, 0)
        left = lane < width
        full = jnp.where(left, covar[:width], covar[width:]) / snaps
        load_lane = jnp.where(left, loading[2 * row], loading[2 * row + 1])
        full = full + jnp.where(lax.rem(lane, width) == r_of, load_lane, 0.0)
        groups = eliminate([full[r : r + SUBS] for r in range(0, width, SUBS)], width - 2, WIDE, 2)
        turned = jnp.concatenate(groups, axis=0).T
        for h in range(2):
            cancels[2 * row + h] = turned[(h + 1) * width - 2 : (h + 1) * width, : width - 2]
        sub, lanes = iota((SUBS, LANES), 0), iota((SUBS, LANES), 1)
        for h in range(2):
            weigh = []
            for k in range(2):
                cols = [-lane_of(value, jnp.full((SUBS, LANES), h * width + width - 2 + k, jnp.int32)) for value in groups]
                cols[-1] = jnp.where(sub < SUBS - 2, cols[-1], jnp.where(sub == SUBS - 2 + k, 1.0, 0.0))
                weigh.append(cols)
            placed = jnp.zeros((SUBS, LANES), jnp.float32)
            for j in range(chunks):
                for k in range(2):
                    total = tree(
                        weigh[k][g] * beams[h][g * SUBS : (g + 1) * SUBS, j * LANES : (j + 1) * LANES]
                        for g in range(width // SUBS)
                    )
                    line = jnp.broadcast_to(jnp.sum(total, axis=0, keepdims=True), (SUBS, LANES))
                    placed = jnp.where(sub == 2 * j + k, line, placed)
            flat[mine + h] = placed
        for to in targets[:2]:
            flat_to(to).start()
        for t in mates:
            cancel_to(t).start()
        for to in targets[2:]:
            flat_to(to).start()

    @pl.when(owner)
    def _():
        arrived(flat, total_panels - 2, send_f, recv_f)
        arrived(cancels, own_panels - 2, send_w, recv_w)
        left_here(codes_got, owners - 1, send_c, recv_c)
        left_here(got, owners - 1, send_a, recv_a)
        left_here(flat, 2 * len(targets), send_f, recv_f)
        left_here(cancels, 2 * len(mates), send_w, recv_w)

    @pl.when(jnp.logical_not(owner))
    def _():
        arrived(flat, total_panels, send_f, recv_f)
        arrived(cancels, own_panels, send_w, recv_w)
        left_here(codes_got, owners, send_c, recv_c)
        left_here(got, owners, send_a, recv_a)


def array_kernel(sizes, flat, cancels, steer, cancel_out, beam_out, out_sem):
    tile_count, total_panels, snaps = sizes
    order = 2 * total_panels
    chunks = snaps // LANES
    count = order // SUBS
    ti = lax.axis_index("tile")
    store = pltpu.make_async_copy(cancels, cancel_out, out_sem)
    store.start()
    parts = [jnp.concatenate([flat[:, 2 * j, :], flat[:, 2 * j + 1, :]], axis=0) for j in range(chunks)]
    joined = jnp.concatenate(parts, axis=1)
    square = (order, LANES)
    lane, r_of = iota(square, 1), iota(square, 0)
    covar = gram(joined) / snaps
    covar = covar + jnp.where(iota((order, order), 0) == iota((order, order), 1), array_load, 0.0)
    full = jnp.concatenate([covar, jnp.zeros((order, LANES - order), jnp.float32)], axis=1)
    full = jnp.where(lane == order, steer[0], jnp.where(lane == order + 1, steer[1], full))
    block = snaps // tile_count
    per = LANES // block
    chunk, spot = lax.div(ti, per), lax.rem(ti, per)
    mine = parts[0]
    for j in range(1, chunks):
        mine = jnp.where(chunk == j, parts[j], mine)
    turned = mine
    for j in range(1, per):
        turned = jnp.where(spot == j, pltpu.roll(mine, LANES - j * block, 1), turned)
    solved = eliminate([full[r : r + SUBS] for r in range(0, order, SUBS)], order, WIDE, 1, (order, order + 1))
    cut = lambda value, g: value[g * SUBS : (g + 1) * SUBS]
    inner = lambda cols, value: jnp.sum(tree(cols[g] * cut(value, g) for g in range(count)), axis=0, keepdims=True)
    s0, s1 = inner(solved[0], turned), inner(solved[1], turned)
    g00, g01 = inner(solved[0], steer[0]), inner(solved[1], steer[0])
    g10, g11 = inner(solved[0], steer[1]), inner(solved[1], steer[1])
    scale = math.sqrt(total_panels) / (g00 * g11 - g01 * g10)
    beam_out[0:1, :] = ((g11 * s0 - g10 * s1) * scale)[:, :block]
    beam_out[1:2, :] = ((g00 * s1 - g01 * s0) * scale)[:, :block]
    store.wait()


def fused_body(panel_count, tile_count, snapshots, beam_codes, panel_codes, loading):
    own_panels, own_tiles, _, snaps = snapshots.shape
    beams_count = beam_codes.shape[0]
    total_panels = own_panels * panel_count
    owners = tile_count // 2
    dma = pltpu.SemaphoreType.DMA
    any_space = pl.BlockSpec(memory_space=pl.ANY)
    vmem = pl.BlockSpec(memory_space=pltpu.VMEM)
    aux = 2 * beams_count - 2
    flat, cancels, steer = pl.pallas_call(
        functools.partial(gather_kernel, (panel_count, tile_count, total_panels)),
        out_shape=(
            pltpu.VMEM((total_panels, 2 * snaps // LANES, LANES), jnp.float32),
            pltpu.VMEM((own_panels, 2, aux), jnp.float32),
            pltpu.VMEM((2, 2 * total_panels, LANES), jnp.float32),
        ),
        in_specs=[any_space] * 4,
        out_specs=(vmem, vmem, vmem),
        scratch_shapes=[
            pltpu.SMEM(loading.shape, loading.dtype),
            pltpu.VMEM((1, total_panels), jnp.int32),
            pltpu.VMEM(snapshots.shape, snapshots.dtype),
            pltpu.VMEM((tile_count, 2, own_tiles, 2, snaps), snapshots.dtype),
            pltpu.VMEM((own_tiles, beams_count), jnp.int32),
            pltpu.VMEM((tile_count, own_tiles, beams_count), jnp.int32),
            dma((4,)),
            dma,
            dma,
            dma,
            dma,
            dma,
            dma,
            dma,
            dma,
        ],
        compiler_params=pltpu.CompilerParams(collective_id=0, has_side_effects=True),
        name="panels",
    )(loading, snapshots, beam_codes.T, panel_codes.reshape(1, -1))
    cancel_t, beam_out = pl.pallas_call(
        functools.partial(array_kernel, (tile_count, total_panels, snaps)),
        out_shape=(
            jax.ShapeDtypeStruct((own_panels, 2, aux), jnp.float32),
            jax.ShapeDtypeStruct((2, snaps // tile_count), jnp.float32),
        ),
        in_specs=[vmem] * 3,
        out_specs=(any_space, vmem),
        scratch_shapes=[dma],
        compiler_params=pltpu.CompilerParams(vmem_limit_bytes=GRANT),
        name="array",
    )(flat, cancels, steer)
    return (jnp.transpose(cancel_t, (0, 2, 1)), beam_out)


def body(mesh_shape, snapshots, beam_codes, panel_codes, loading):
    panel_count, tile_count = mesh_shape
    own_panels, own_tiles, _, snaps = snapshots.shape
    block = snaps // tile_count
    fits = (
        own_panels == tile_count
        and tile_count % 2 == 0
        and tile_count >= 4
        and own_tiles % SUBS == 0
        and 4 * beam_codes.shape[0] == LANES
        and (2 * own_panels * panel_count) % (WIDE * SUBS) == 0
        and 2 * own_panels * panel_count + 2 <= LANES
        and 2 * snaps == SUBS * LANES
        and block <= LANES
        and LANES % block == 0
    )
    if not fits:
        return plain_body(snapshots, beam_codes, panel_codes, loading)
    return fused_body(panel_count, tile_count, snapshots, beam_codes, panel_codes, loading)


def solution(mesh):
    placed = (P("panel", "tile", None, None), P(None, "tile"), P(), P("panel"))
    return jax.shard_map(
        functools.partial(body, (mesh.shape["panel"], mesh.shape["tile"])),
        mesh=mesh,
        in_specs=placed,
        out_specs=(P("panel", None, None), P(None, "tile")),
        check_vma=False,
    )
```
